32 devices in a mesh: groups: 2 (over y), rows: 4 (over z), cols: 2 (over x), sub: 2 (over core).
Axes of the slice: x: 2, y: 2, z: 4, core: 2. Of those that a mesh axis runs over, the one named last changes fastest.
Arguments:
- diagonal_tiles: float32 [256, 128, 128], P(('groups', 'rows', 'sub')), parts along dimension 0
- coupling_tiles: float32 [256, 6, 128, 128], P(('groups', 'rows', 'sub'), 'cols'), parts along dimension 0, may hold values from -0.0625 to 0.0625
- column_part: int32 [256, 6], P(('groups', 'rows', 'sub'), 'cols'), parts along dimension 0, may hold values from 0 to 4
- column_tile: int32 [256, 6], P(('groups', 'rows', 'sub'), 'cols'), parts along dimension 0, may hold values from 0 to 31
- neighbours: int32 [8, 4], P('groups'), parts along dimension 0, may hold values from 0 to 3, as said below
- right_side: float32 [256, 128], P(('groups', 'rows', 'sub')), parts along dimension 0, may hold values from -6 to 6
- jacobi_inverse: float32 [256, 128, 128], P(('groups', 'rows', 'sub')), parts along dimension 0, as said below
Outputs:
- solution: float32 [256, 128], P(('groups', 'rows', 'sub')), parts along dimension 0
- residual: float32 [256, 128], P(('groups', 'rows', 'sub')), parts along dimension 0
The draws below stay inside these ranges and needn't reach their ends.
There are 2 independent parts, one for each index of `groups`. The reference program is written for one: setup_inputs(seed, part) draws one part's arguments, and reference() takes and returns one part's arrays. A program takes and returns all parts, laid end to end along the dimension named above; each array names one. Nothing has to cross between parts.
Inputs may be any that keep to these rules, and one draw needn't show every extreme that they name: `neighbours`: entry 0 of partition p's list is (p + 4 // 2) mod 4, the opposite partition on the cycle; every other entry names a partition whose index differs from p by 1 to 2 (without wrapping round); entries may repeat. `jacobi_inverse`: block-diagonal: each group of 5 consecutive variables, from the first on, forms one 5 x 5 block, and each variable left over after the last whole group of 5 is a 1 x 1 block of its own.
All inputs are finite; a program needn't handle non-finite values.
Results may differ from the reference program's by a relative error of at most 0.00019.
Values sent between devices are 32-bit elements; how exact they have to be, the bound alone decides.
A program may use at most 64 MiB of HBM per device.

```python
import jax
import jax.numpy as jnp
from jax import lax

TW = 128
NR = 2
ITERS = 2
RB = 32
NB = 128
K = 6
NNB = 4
N_ROWS = 4


def draw_diagonal_tiles(key, part):
    first, second = jax.random.split(jax.random.fold_in(key, 11))
    scales = jax.random.uniform(first, (NB, TW, 1), jnp.float32, 1.5, 2.5)
    noise = jax.random.normal(second, (NB, TW, TW), jnp.float32)
    return scales * jnp.eye(TW, dtype=jnp.float32) + 0.3 / TW ** 0.5 * noise


def draw_jacobi_inverse(key, part):
    first, second = jax.random.split(jax.random.fold_in(key, 23))
    index = jnp.arange(TW, dtype=jnp.int32)
    cutoff = TW // 5 * 5
    blocks = jnp.where(index < cutoff, index // 5, TW + index)
    inside = (blocks[:, None] == blocks[None, :]).astype(jnp.float32)
    scales = jax.random.uniform(first, (NB, TW, 1), jnp.float32, 0.4, 1.0)
    noise = jax.random.normal(second, (NB, TW, TW), jnp.float32) * 0.15
    return (scales * jnp.eye(TW, dtype=jnp.float32) + noise) * inside


def draw_neighbours(key, part):
    picked = jax.random.randint(jax.random.fold_in(key, 37), (N_ROWS, NNB), 0, NNB)
    offset = jnp.where(picked < NR, picked - NR, picked - NR + 1)
    owner = jnp.arange(N_ROWS, dtype=jnp.int32)[:, None]
    target = owner + offset
    target = jnp.where((target < 0) | (target >= N_ROWS), owner - offset, target)
    opposite = (owner + N_ROWS // 2) % N_ROWS
    column = jnp.arange(NNB, dtype=jnp.int32)[None, :]
    target = jnp.where(column == 0, opposite, target)
    return target.astype(jnp.int32)


def set_ends(entries, key, smallest, largest):
    dims = entries.shape
    index_at = [jax.random.randint(jax.random.fold_in(key, axis), (), 0, dims[axis]) for axis in range(len(dims))]
    entries = entries.at[tuple(index_at)].set(smallest)
    longest = dims.index(max(dims))
    index_at[longest] = (index_at[longest] + 1) % dims[longest]
    return entries.at[tuple(index_at)].set(largest)


def level_of(key, dims, shards, least, largest):
    level = 1.0
    for axis_at, parts in shards:
        steps = jax.random.uniform(jax.random.fold_in(jax.random.fold_in(key, 6), axis_at), (parts,), jnp.float32, least / len(shards), largest / len(shards))
        level = level * jnp.repeat(jnp.exp(steps), dims[axis_at] // parts).reshape((-1,) + (1,) * (len(dims) - 1 - axis_at))
    return level


def gaussian(own_key, extent, deviation, limit, cuts=(), kind=jnp.bfloat16):
    result = deviation * jax.random.normal(own_key, extent, jnp.float32)
    if cuts:
        result = result * level_of(own_key, extent, cuts, -0.22, 0.18)
    return jnp.clip(result, -limit, limit).astype(kind)


def setup_inputs(seed: int = 0, part: int = 0) -> dict:
    splits = jax.random.split(jax.random.key(seed), 8)
    part_splits = jax.random.split(jax.random.fold_in(splits[7], part), 8)
    diagonal_tiles = draw_diagonal_tiles(jax.random.fold_in(jax.random.fold_in(splits[7], part), 71), part)
    coupling_tiles = gaussian(part_splits[1], (NB, K, TW, TW), (11 * K * TW) ** -0.5, 0.0625, ((0, 8), (1, 2)), jnp.float32)
    column_part = set_ends(jax.random.randint(part_splits[2], (NB, K), 0, NNB + 1), jax.random.fold_in(part_splits[2], 1), 0, NNB).astype(jnp.int32)
    column_tile = set_ends(jax.random.randint(part_splits[3], (NB, K), 0, RB), jax.random.fold_in(part_splits[3], 1), 0, RB - 1).astype(jnp.int32)
    neighbours = draw_neighbours(jax.random.fold_in(jax.random.fold_in(splits[7], part), 71), part)
    right_side = gaussian(part_splits[5], (NB, TW), 1.0, 6.0, ((0, 8),), jnp.float32)
    jacobi_inverse = draw_jacobi_inverse(jax.random.fold_in(jax.random.fold_in(splits[7], part), 71), part)
    return dict(diagonal_tiles=diagonal_tiles, coupling_tiles=coupling_tiles, column_part=column_part, column_tile=column_tile, neighbours=neighbours, right_side=right_side, jacobi_inverse=jacobi_inverse)


def transpose_apply(vector, diagonal_tiles, coupling_tiles, column_part, column_tile, neighbours):
    highest = lax.Precision.HIGHEST
    diagonal_part = jnp.einsum('rij,ri->rj', diagonal_tiles, vector, precision=highest)
    partial_value = jnp.einsum('rkij,ri->rkj', coupling_tiles, vector, precision=highest)
    tile_rows = vector.shape[0]
    part_rows = tile_rows // N_ROWS
    owner = jnp.arange(tile_rows, dtype=jnp.int32) // part_rows
    listed = neighbours[owner]
    chosen = jnp.take_along_axis(listed, jnp.maximum(column_part - 1, 0).astype(jnp.int32), axis=1)
    target = jnp.where(column_part == 0, owner[:, None], chosen)
    landing = (target * part_rows + column_tile).astype(jnp.int32).reshape(-1)
    summed = jax.ops.segment_sum(partial_value.reshape(-1, partial_value.shape[-1]), landing, num_segments=tile_rows)
    return diagonal_part + summed


def precondition(jacobi_inverse, vector):
    return jnp.einsum('rij,ri->rj', jacobi_inverse, vector, precision=lax.Precision.HIGHEST)


def reference(diagonal_tiles, coupling_tiles, column_part, column_tile, neighbours, right_side, jacobi_inverse):
    def apply_a(vector):
        return transpose_apply(vector, diagonal_tiles, coupling_tiles, column_part, column_tile, neighbours)

    solution = jnp.zeros_like(right_side)
    residual = right_side
    shadow = right_side
    search = right_side
    rho_now = jnp.sum(shadow * residual)
    for step in range(ITERS):
        search_hat = precondition(jacobi_inverse, search)
        image = apply_a(search_hat)
        alpha = rho_now / jnp.sum(shadow * image)
        half = residual - alpha * image
        half_hat = precondition(jacobi_inverse, half)
        twice = apply_a(half_hat)
        omega = jnp.sum(twice * half) / jnp.sum(twice * twice)
        solution = solution + alpha * search_hat + omega * half_hat
        residual = half - omega * twice
        if step + 1 < ITERS:
            rho_next = jnp.sum(shadow * residual)
            search = residual + (rho_next / rho_now) * (alpha / omega) * (search - omega * image)
            rho_now = rho_next
    return solution, residual
```

```python
import functools

import jax
import jax.numpy as jnp
from jax import lax
from jax.experimental import pallas as pl
from jax.experimental.pallas import tpu as pltpu
from jax.sharding import PartitionSpec as P

MESH = pl.DeviceIdType.MESH
REACH = 2
APPLIES = 4
SUBLANES = 8
F32 = jnp.float32


def offsets_of(count):
    wanted = {d % count for d in range(-REACH, REACH + 1)} | {count // 2}
    return sorted(wanted)


def kernel(
    sizes,
    diag_hbm,
    coup_hbm,
    jac_hbm,
    part_ref,
    tile_ref,
    near_ref,
    right_ref,
    sol_ref,
    res_ref,
    diag,
    coup,
    jac,
    one_hot,
    prod,
    dprod,
    vec,
    landed,
    pair_recv,
    owned,
    recv,
    dots,
    dots_recv,
    load_sem,
    pair_send_sem,
    pair_recv_sem,
    send_sem,
    recv_sem,
    dots_send_sem,
    dots_recv_sem,
):
    n_rows, n_cols, n_sub = sizes
    offsets = offsets_of(n_rows)
    slots = len(offsets)
    rows_dev, slot_count, width, _ = coup.shape
    half_rows = slots * rows_dev
    chunk = rows_dev * SUBLANES
    row = lax.axis_index("rows")
    col = lax.axis_index("cols")
    sub = lax.axis_index("sub")
    me = row * n_sub + sub
    twin = n_sub - 1 - sub

    loads = [
        pltpu.make_async_copy(jac_hbm, jac, load_sem.at[0]),
        pltpu.make_async_copy(diag_hbm, diag, load_sem.at[1]),
        pltpu.make_async_copy(coup_hbm, coup, load_sem.at[2]),
    ]
    for load in loads:
        load.start()

    def partner(slot):
        return lax.rem(row + offsets[slot], n_rows)

    def if_linked(slot, act):
        if offsets[slot] in (0, n_rows // 2):
            act()
        else:
            pl.when(jnp.abs(partner(slot) - row) <= REACH)(act)

    barrier = pltpu.get_barrier_semaphore()

    def dot_peers():
        for step in range(1, n_rows * n_sub):
            peer = lax.rem(me + step, n_rows * n_sub)
            yield step, peer, {"rows": lax.div(peer, n_sub), "cols": col, "sub": lax.rem(peer, n_sub)}

    recv[...] = jnp.zeros_like(recv)
    dots[...] = jnp.zeros_like(dots)
    for _, _, where in dot_peers():
        pl.semaphore_signal(barrier, inc=1, device_id=where, device_id_type=MESH)
    for slot in range(slots):
        for step in range(1, n_cols):
            where = {"rows": partner(slot), "cols": lax.rem(col + step, n_cols), "sub": sub}

            def greet(where=where):
                pl.semaphore_signal(barrier, inc=1, device_id=where, device_id_type=MESH)

            if_linked(slot, greet)

    part = part_ref[...]
    tile = tile_ref[...]
    target = jnp.full(part.shape, row, jnp.int32)
    for j in range(near_ref.shape[1]):
        target = jnp.where(part == j + 1, near_ref[row, j], target)
    apart = target - row
    apart = jnp.where(apart < 0, apart + n_rows, apart)
    place = jnp.zeros(part.shape, jnp.int32)
    for slot in range(1, slots):
        place = jnp.where(apart == offsets[slot], slot, place)
    landing = place * rows_dev + tile
    for j in range(1, n_sub):
        landing = jnp.where(tile >= j * rows_dev, landing + (half_rows - rows_dev), landing)
    lanes = -(-n_sub * half_rows // 128) * 128
    lane = lax.broadcasted_iota(jnp.int32, (rows_dev, lanes), 1)
    for k in range(slot_count):
        hit = (landing[:, k : k + 1] == lane).astype(F32)
        hit = jnp.broadcast_to(hit[:, None, :], (rows_dev, SUBLANES, lanes)).reshape(chunk, lanes)
        turned = jnp.transpose(hit)[: n_sub * half_rows]
        one_hot[:, k * chunk : (k + 1) * chunk] = turned.astype(jnp.bfloat16)

    loads[0].wait()

    def turn(r, carry):
        jac[r] = jnp.transpose(jac[r])
        return carry

    lax.fori_loop(0, rows_dev, turn, 0, unroll=4)

    def pair_copy(e):
        return pltpu.make_async_remote_copy(
            src_ref=landed.at[e, pl.ds(pl.multiple_of(twin * half_rows, rows_dev), half_rows)],
            dst_ref=pair_recv.at[e],
            send_sem=pair_send_sem.at[e],
            recv_sem=pair_recv_sem.at[e],
            device_id={"sub": twin},
            device_id_type=MESH,
        )

    def owner_copy(e, slot, step):
        back = offsets.index(-offsets[slot] % n_rows)
        return pltpu.make_async_remote_copy(
            src_ref=owned.at[e, pl.ds(slot * rows_dev, rows_dev)],
            dst_ref=recv.at[e, back, col],
            send_sem=send_sem.at[e, slot, step],
            recv_sem=recv_sem.at[e, back, col],
            device_id={"rows": partner(slot), "cols": lax.rem(col + step, n_cols)},
            device_id_type=MESH,
        )

    def owner_arrival(e, slot, step):
        source = lax.rem(col + step, n_cols)
        return pltpu.make_async_remote_copy(
            src_ref=owned.at[e, pl.ds(slot * rows_dev, rows_dev)],
            dst_ref=recv.at[e, slot, source],
            send_sem=send_sem.at[e, slot, step],
            recv_sem=recv_sem.at[e, slot, source],
            device_id={"rows": partner(slot), "cols": source},
            device_id_type=MESH,
        )

    routes = [(s, c) for s in range(slots) for c in range(n_cols) if (s, c) != (0, 0)]

    def each_route(act):
        for slot, step in routes:
            if_linked(slot, functools.partial(act, slot, step))

    def dots_copy(e, step, peer, where):
        return pltpu.make_async_remote_copy(
            src_ref=dots.at[e],
            dst_ref=dots_recv.at[e, me],
            send_sem=dots_send_sem.at[e, step],
            recv_sem=dots_recv_sem.at[e, me],
            device_id=where,
            device_id_type=MESH,
        )

    def dots_start(e, products):
        for j, product in enumerate(products):
            dots[e, j : j + 1] = jnp.sum(product, axis=0, keepdims=True)
        for step, peer, where in dot_peers():
            dots_copy(e, step, peer, where).start()
        dots_recv[e, me] = dots[e]

    def dots_finish(e, count):
        for step, peer, where in dot_peers():
            pltpu.make_async_remote_copy(
                src_ref=dots.at[e],
                dst_ref=dots_recv.at[e, peer],
                send_sem=dots_send_sem.at[e, step],
                recv_sem=dots_recv_sem.at[e, peer],
                device_id=where,
                device_id_type=MESH,
            ).wait_recv()
        total = jnp.sum(dots_recv[e], axis=0)
        total = jnp.broadcast_to(jnp.sum(total, axis=1, keepdims=True), total.shape)
        return [total[j : j + 1] for j in range(count)]

    def fold(product):
        return jnp.sum(product.reshape(width // SUBLANES, SUBLANES, width), axis=0)

    unroll = 4 if rows_dev % 4 == 0 else 1

    def apply(e, value):
        vec[e] = value
        if e == 0:
            loads[1].wait()
            loads[2].wait()

        def some_rows(g, carry):
            for u in range(unroll):
                r = g * unroll + u
                hat = jnp.sum(jac[r] * vec[e, pl.ds(r, 1)], axis=1, keepdims=True)
                hat = jnp.broadcast_to(hat, (width, width))
                for k in range(slot_count):
                    at = pl.multiple_of(k * chunk + r * SUBLANES, SUBLANES)
                    prod[pl.ds(at, SUBLANES)] = fold(coup[r, k] * hat)
                dprod[pl.ds(pl.multiple_of(r * SUBLANES, SUBLANES), SUBLANES)] = fold(diag[r] * hat)
            return carry

        lax.fori_loop(0, rows_dev // unroll, some_rows, 0)
        rest = prod[...]
        out = None
        for _ in range(3):
            piece = rest.astype(jnp.bfloat16)
            rest = rest - piece.astype(F32)
            term = jnp.dot(one_hot[...], piece, preferred_element_type=F32)
            out = term if out is None else out + term
        landed[e] = out
        if e == 0:
            greetings = n_rows * n_sub - 1
            for slot in range(slots):
                linked = 1
                if offsets[slot] not in (0, n_rows // 2):
                    linked = (jnp.abs(partner(slot) - row) <= REACH).astype(jnp.int32)
                greetings = greetings + (n_cols - 1) * linked
            pl.semaphore_wait(barrier, greetings)
        pair_copy(e).start()
        pair_copy(e).wait_recv()
        mine = landed[e, pl.ds(pl.multiple_of(sub * half_rows, rows_dev), half_rows)]
        owned[e] = mine + pair_recv[e]
        each_route(lambda slot, step: owner_copy(e, slot, step).start())
        recv[e, 0, col] = owned[e, :rows_dev]
        own = jnp.sum(dprod[...].reshape(rows_dev, SUBLANES, width), axis=1)
        each_route(lambda slot, step: owner_arrival(e, slot, step).wait_recv())
        for slot in range(slots):
            for c in range(n_cols):
                own = own + recv[e, slot, c]
        return own

    shadow = right_ref[...]
    image = apply(0, shadow)
    dots_start(0, [shadow * shadow, shadow * image])
    second = apply(1, image)
    rho, shadow_image = dots_finish(0, 2)
    alpha = rho / shadow_image
    half = shadow - alpha * image
    twice = image - alpha * second
    dots_start(1, [twice * half, twice * twice, shadow * half, shadow * twice])
    third = apply(2, twice)
    cross, square, shadow_half, shadow_twice = dots_finish(1, 4)
    omega = cross / square
    rho_next = shadow_half - omega * shadow_twice
    beta = rho_next / rho * (alpha / omega)
    residual = half - omega * twice
    search = residual + beta * (shadow - omega * image)
    residual_image = twice - omega * third
    image = residual_image + beta * (image - omega * second)
    dots_start(2, [shadow * image])
    fourth = apply(3, image)
    alpha_next = rho_next / dots_finish(2, 1)[0]
    half_next = residual - alpha_next * image
    twice = residual_image - alpha_next * fourth
    dots_start(3, [twice * half_next, twice * twice])

    vec[0] = alpha * shadow + omega * half + alpha_next * search
    vec[1] = half_next
    at_lane = lax.broadcasted_iota(jnp.int32, (width, width), 1)

    def hats(r, carry):
        for j in range(2):
            hat = jnp.sum(jac[r] * vec[j, pl.ds(r, 1)], axis=1, keepdims=True)
            carry = jnp.where(at_lane == j * rows_dev + r, hat, carry)
        return carry

    hat = lax.fori_loop(0, rows_dev, hats, jnp.zeros((width, width), F32), unroll=4)
    hat = jnp.transpose(hat)
    cross, square = dots_finish(3, 2)
    omega = cross / square
    sol_ref[...] = hat[:rows_dev] + omega * hat[rows_dev : 2 * rows_dev]
    res_ref[...] = half_next - omega * twice

    for e in range(APPLIES):
        pair_copy(e).wait_send()
        each_route(lambda slot, step: owner_copy(e, slot, step).wait_send())
        for step, peer, where in dot_peers():
            dots_copy(e, step, peer, where).wait_send()


def on_device(
    diagonal_tiles, coupling_tiles, column_part, column_tile, neighbours, right_side, jacobi_inverse
):
    n_rows, n_cols, n_sub = (lax.axis_size(a) for a in ("rows", "cols", "sub"))
    slots = len(offsets_of(n_rows))
    rows_dev, slot_count, width, _ = coupling_tiles.shape
    half_rows = slots * rows_dev
    chunk = rows_dev * SUBLANES
    peers = n_rows * n_sub
    hbm = pl.BlockSpec(memory_space=pl.ANY)
    vmem = pl.BlockSpec(memory_space=pltpu.VMEM)
    dma = pltpu.SemaphoreType.DMA
    scratch = [
        pltpu.VMEM(diagonal_tiles.shape, F32),
        pltpu.VMEM(coupling_tiles.shape, F32),
        pltpu.VMEM(jacobi_inverse.shape, F32),
        pltpu.VMEM((n_sub * half_rows, slot_count * chunk), jnp.bfloat16),
        pltpu.VMEM((slot_count * chunk, width), F32),
        pltpu.VMEM((chunk, width), F32),
        pltpu.VMEM((APPLIES, rows_dev, width), F32),
        pltpu.VMEM((APPLIES, n_sub * half_rows, width), F32),
        pltpu.VMEM((APPLIES, half_rows, width), F32),
        pltpu.VMEM((APPLIES, half_rows, width), F32),
        pltpu.VMEM((APPLIES, slots, n_cols, rows_dev, width), F32),
        pltpu.VMEM((APPLIES, SUBLANES, width), F32),
        pltpu.VMEM((APPLIES, peers, SUBLANES, width), F32),
        dma((3,)),
        dma((APPLIES,)),
        dma((APPLIES,)),
        dma((APPLIES, slots, n_cols)),
        dma((APPLIES, slots, n_cols)),
        dma((APPLIES, peers)),
        dma((APPLIES, peers)),
    ]
    out = jax.ShapeDtypeStruct(right_side.shape, F32)
    return pl.pallas_call(
        functools.partial(kernel, (n_rows, n_cols, n_sub)),
        out_shape=(out, out),
        in_specs=[hbm, hbm, hbm, vmem, vmem, pl.BlockSpec(memory_space=pltpu.SMEM), vmem],
        out_specs=(vmem, vmem),
        scratch_shapes=scratch,
        compiler_params=pltpu.CompilerParams(
            collective_id=0, has_side_effects=True, vmem_limit_bytes=56 * 2**20
        ),
        name="solve",
    )(diagonal_tiles, coupling_tiles, jacobi_inverse, column_part, column_tile, neighbours, right_side)


def solution(mesh):
    in_specs = (
        P(("groups", "rows", "sub"), None, None),
        P(("groups", "rows", "sub"), "cols", None, None),
        P(("groups", "rows", "sub"), "cols"),
        P(("groups", "rows", "sub"), "cols"),
        P("groups", None),
        P(("groups", "rows", "sub"), None),
        P(("groups", "rows", "sub"), None, None),
    )
    out_specs = (P(("groups", "rows", "sub"), None), P(("groups", "rows", "sub"), None))
    return jax.shard_map(
        on_device, mesh=mesh, in_specs=in_specs, out_specs=out_specs, check_vma=False
    )
```

```python
import functools

import jax
import jax.numpy as jnp
from jax import lax
from jax.experimental import pallas as pl
from jax.experimental.pallas import tpu as pltpu
from jax.sharding import PartitionSpec as P

MESH = pl.DeviceIdType.MESH
REACH = 2
APPLIES = 4
SUBLANES = 8
F32 = jnp.float32


def offsets_of(count):
    wanted = {d % count for d in range(-REACH, REACH + 1)} | {count // 2}
    return sorted(wanted)


def kernel(
    sizes,
    diag_hbm,
    coup_hbm,
    jac_hbm,
    part_ref,
    tile_ref,
    near_ref,
    right_ref,
    out_ref,
    diag,
    coup,
    jac,
    one_hot,
    prod,
    dprod,
    vec,
    landed,
    recv,
    dots,
    dots_recv,
    load_sem,
    send_sem,
    recv_sem,
    dots_send_sem,
    dots_recv_sem,
):
    n_rows, n_cols, n_sub = sizes
    offsets = offsets_of(n_rows)
    slots = len(offsets)
    rows_dev, slot_count, width, _ = coup.shape
    half_rows = slots * rows_dev
    chunk = rows_dev * SUBLANES
    row = lax.axis_index("rows")
    col = lax.axis_index("cols")
    sub = lax.axis_index("sub")
    me = row * n_sub + sub

    loads = [
        pltpu.make_async_copy(jac_hbm, jac, load_sem.at[0]),
        pltpu.make_async_copy(diag_hbm, diag, load_sem.at[1]),
        pltpu.make_async_copy(coup_hbm, coup, load_sem.at[2]),
    ]
    for load in loads:
        load.start()

    def partner(slot):
        return lax.rem(row + offsets[slot], n_rows)

    def if_linked(slot, act):
        if offsets[slot] in (0, n_rows // 2):
            act()
        else:
            pl.when(jnp.abs(partner(slot) - row) <= REACH)(act)

    def corner(slot, step):
        return {
            "rows": partner(slot),
            "cols": lax.rem(col + step // n_sub, n_cols),
            "sub": lax.rem(sub + step % n_sub, n_sub),
        }

    barrier = pltpu.get_barrier_semaphore()

    def dot_peers():
        for step in range(1, n_rows * n_sub):
            peer = lax.rem(me + step, n_rows * n_sub)
            yield step, peer, {"rows": lax.div(peer, n_sub), "cols": col, "sub": lax.rem(peer, n_sub)}

    recv[...] = jnp.zeros_like(recv)
    for _, _, where in dot_peers():
        pl.semaphore_signal(barrier, inc=1, device_id=where, device_id_type=MESH)
    for slot in range(slots):
        for step in range(n_sub, n_cols * n_sub):

            def greet(slot=slot, step=step):
                where = corner(slot, step)
                pl.semaphore_signal(barrier, inc=1, device_id=where, device_id_type=MESH)

            if_linked(slot, greet)

    part = part_ref[...]
    tile = tile_ref[...]
    target = jnp.full(part.shape, row, jnp.int32)
    for j in range(near_ref.shape[1]):
        target = jnp.where(part == j + 1, near_ref[row, j], target)
    apart = target - row
    apart = jnp.where(apart < 0, apart + n_rows, apart)
    place = jnp.zeros(part.shape, jnp.int32)
    for slot in range(1, slots):
        place = jnp.where(apart == offsets[slot], slot, place)
    landing = place * rows_dev + tile
    for j in range(1, n_sub):
        landing = jnp.where(tile >= j * rows_dev, landing + (half_rows - rows_dev), landing)
    from_row = lax.broadcasted_iota(jnp.int32, (rows_dev, chunk), 0)
    to_lane = lax.broadcasted_iota(jnp.int32, (rows_dev, chunk), 1)
    first = from_row * SUBLANES
    spread = ((to_lane >= first) & (to_lane < first + SUBLANES)).astype(F32)
    spread_landing = jnp.dot(
        landing.astype(F32), spread, precision=lax.Precision.HIGHEST, preferred_element_type=F32
    )
    at_row = lax.broadcasted_iota(jnp.int32, (n_sub * half_rows, chunk), 0).astype(F32)
    for k in range(slot_count):
        hit = (spread_landing[k : k + 1] == at_row).astype(F32)
        one_hot[:, k * chunk : (k + 1) * chunk] = hit.astype(jnp.bfloat16)

    loads[0].wait()

    def turn(r, carry):
        jac[r] = jnp.transpose(jac[r])
        return carry

    lax.fori_loop(0, rows_dev, turn, 0, unroll=4)

    def block(e, slot, to_sub):
        at = pl.multiple_of(to_sub * half_rows + slot * rows_dev, rows_dev)
        return landed.at[e, pl.ds(at, rows_dev)]

    def owner_copy(e, slot, step):
        back = offsets.index(-offsets[slot] % n_rows)
        where = corner(slot, step)
        return pltpu.make_async_remote_copy(
            src_ref=block(e, slot, where["sub"]),
            dst_ref=recv.at[e, back, col, sub],
            send_sem=send_sem.at[e, slot, step],
            recv_sem=recv_sem.at[e, back, col, sub],
            device_id=where,
            device_id_type=MESH,
        )

    def owner_arrival(e, slot, step):
        where = corner(slot, step)
        return pltpu.make_async_remote_copy(
            src_ref=block(e, slot, where["sub"]),
            dst_ref=recv.at[e, slot, where["cols"], where["sub"]],
            send_sem=send_sem.at[e, slot, step],
            recv_sem=recv_sem.at[e, slot, where["cols"], where["sub"]],
            device_id=where,
            device_id_type=MESH,
        )

    far_first = sorted(range(slots), key=lambda s: -min(offsets[s], n_rows - offsets[s]))
    routes = [(s, c) for s in far_first for c in reversed(range(n_cols * n_sub)) if (s, c) != (0, 0)]

    def each_route(act):
        for slot, step in routes:
            if_linked(slot, functools.partial(act, slot, step))

    def dots_copy(e, step, peer, where):
        return pltpu.make_async_remote_copy(
            src_ref=dots.at[e],
            dst_ref=dots_recv.at[e, pl.ds(me, 1)],
            send_sem=dots_send_sem.at[e, step],
            recv_sem=dots_recv_sem.at[e, me],
            device_id=where,
            device_id_type=MESH,
        )

    def dots_start(e, products):
        at = lax.broadcasted_iota(jnp.int32, (1, width), 1)
        line = jnp.zeros((1, width), F32)
        for j, product in enumerate(products):
            total = jnp.sum(jnp.sum(product, axis=0, keepdims=True), axis=1, keepdims=True)
            line = jnp.where(at == j, total, line)
        dots[e] = line
        for step, peer, where in dot_peers():
            dots_copy(e, step, peer, where).start()
        dots_recv[e, pl.ds(me, 1)] = line

    def dots_finish(e, count):
        for step, peer, where in dot_peers():
            pltpu.make_async_remote_copy(
                src_ref=dots.at[e],
                dst_ref=dots_recv.at[e, pl.ds(peer, 1)],
                send_sem=dots_send_sem.at[e, step],
                recv_sem=dots_recv_sem.at[e, peer],
                device_id=where,
                device_id_type=MESH,
            ).wait_recv()
        total = jnp.sum(dots_recv[e], axis=0, keepdims=True)
        return [jnp.broadcast_to(total[:, j : j + 1], total.shape) for j in range(count)]

    def fold(product):
        return jnp.sum(product.reshape(width // SUBLANES, SUBLANES, width), axis=0)

    unroll = 4 if rows_dev % 4 == 0 else 1

    def apply(e, value):
        vec[e] = value
        if e == 0:
            loads[1].wait()
            loads[2].wait()

        def some_rows(g, carry):
            for u in range(unroll):
                r = g * unroll + u
                hat = jnp.sum(jac[r] * vec[e, pl.ds(r, 1)], axis=1, keepdims=True)
                hat = jnp.broadcast_to(hat, (width, width))
                for k in range(slot_count):
                    at = pl.multiple_of(k * chunk + r * SUBLANES, SUBLANES)
                    prod[pl.ds(at, SUBLANES)] = fold(coup[r, k] * hat)
                dprod[pl.ds(pl.multiple_of(r * SUBLANES, SUBLANES), SUBLANES)] = fold(diag[r] * hat)
            return carry

        lax.fori_loop(0, rows_dev // unroll, some_rows, 0)
        rest = prod[...]
        out = None
        for _ in range(3):
            piece = rest.astype(jnp.bfloat16)
            rest = rest - piece.astype(F32)
            term = jnp.dot(one_hot[...], piece, preferred_element_type=F32)
            out = term if out is None else out + term
        landed[e] = out
        if e == 0:
            greetings = n_rows * n_sub - 1
            for slot in range(slots):
                linked = 1
                if offsets[slot] not in (0, n_rows // 2):
                    linked = (jnp.abs(partner(slot) - row) <= REACH).astype(jnp.int32)
                greetings = greetings + (n_cols - 1) * n_sub * linked
            pl.semaphore_wait(barrier, greetings)
        each_route(lambda slot, step: owner_copy(e, slot, step).start())
        recv[e, 0, col, sub] = landed[e, pl.ds(pl.multiple_of(sub * half_rows, rows_dev), rows_dev)]
        own = jnp.sum(dprod[...].reshape(rows_dev, SUBLANES, width), axis=1)
        each_route(lambda slot, step: owner_arrival(e, slot, step).wait_recv())
        for slot in range(slots):
            for c in range(n_cols):
                for s in range(n_sub):
                    own = own + recv[e, slot, c, s]
        return own

    shadow = right_ref[...]
    image = apply(0, shadow)
    dots_start(0, [shadow * shadow, shadow * image])
    second = apply(1, image)
    rho, shadow_image = dots_finish(0, 2)
    alpha = rho / shadow_image
    half = shadow - alpha * image
    twice = image - alpha * second
    dots_start(1, [twice * half, twice * twice, shadow * half, shadow * twice])
    third = apply(2, twice)
    cross, square, shadow_half, shadow_twice = dots_finish(1, 4)
    omega = cross / square
    rho_next = shadow_half - omega * shadow_twice
    beta = rho_next / rho * (alpha / omega)
    residual = half - omega * twice
    search = residual + beta * (shadow - omega * image)
    residual_image = twice - omega * third
    image = residual_image + beta * (image - omega * second)
    dots_start(2, [shadow * image])
    fourth = apply(3, image)
    alpha_next = rho_next / dots_finish(2, 1)[0]
    half_next = residual - alpha_next * image
    twice = residual_image - alpha_next * fourth
    dots_start(3, [twice * half_next, twice * twice])

    vec[0] = alpha * shadow + omega * half + alpha_next * search
    vec[1] = half_next
    at_lane = lax.broadcasted_iota(jnp.int32, (width, width), 1)

    def hats(r, carry):
        for j in range(2):
            hat = jnp.sum(jac[r] * vec[j, pl.ds(r, 1)], axis=1, keepdims=True)
            carry = jnp.where(at_lane == j * rows_dev + r, hat, carry)
        return carry

    hat = lax.fori_loop(0, rows_dev, hats, jnp.zeros((width, width), F32), unroll=4)
    hat = jnp.transpose(hat)
    cross, square = dots_finish(3, 2)
    omega = cross / square
    out_ref[:rows_dev] = hat[:rows_dev] + omega * hat[rows_dev : 2 * rows_dev]
    out_ref[rows_dev:] = half_next - omega * twice

    for e in range(APPLIES):
        each_route(lambda slot, step: owner_copy(e, slot, step).wait_send())
        for step, peer, where in dot_peers():
            dots_copy(e, step, peer, where).wait_send()


def split(both_ref, sol_ref, res_ref):
    rows_dev = sol_ref.shape[0]
    sol_ref[...] = both_ref[:rows_dev]
    res_ref[...] = both_ref[rows_dev:]


def on_device(
    diagonal_tiles, coupling_tiles, column_part, column_tile, neighbours, right_side, jacobi_inverse
):
    n_rows, n_cols, n_sub = (lax.axis_size(a) for a in ("rows", "cols", "sub"))
    slots = len(offsets_of(n_rows))
    rows_dev, slot_count, width, _ = coupling_tiles.shape
    half_rows = slots * rows_dev
    chunk = rows_dev * SUBLANES
    peers = n_rows * n_sub
    hbm = pl.BlockSpec(memory_space=pl.ANY)
    vmem = pl.BlockSpec(memory_space=pltpu.VMEM)
    dma = pltpu.SemaphoreType.DMA
    scratch = [
        pltpu.VMEM(diagonal_tiles.shape, F32),
        pltpu.VMEM(coupling_tiles.shape, F32),
        pltpu.VMEM(jacobi_inverse.shape, F32),
        pltpu.VMEM((n_sub * half_rows, slot_count * chunk), jnp.bfloat16),
        pltpu.VMEM((slot_count * chunk, width), F32),
        pltpu.VMEM((chunk, width), F32),
        pltpu.VMEM((APPLIES, rows_dev, width), F32),
        pltpu.VMEM((APPLIES, n_sub * half_rows, width), F32),
        pltpu.VMEM((APPLIES, slots, n_cols, n_sub, rows_dev, width), F32),
        pltpu.VMEM((APPLIES, 1, width), F32),
        pltpu.VMEM((APPLIES, peers, width), F32),
        dma((3,)),
        dma((APPLIES, slots, n_cols * n_sub)),
        dma((APPLIES, slots, n_cols, n_sub)),
        dma((APPLIES, peers)),
        dma((APPLIES, peers)),
    ]
    both = pl.pallas_call(
        functools.partial(kernel, (n_rows, n_cols, n_sub)),
        out_shape=jax.ShapeDtypeStruct((2 * rows_dev, width), F32),
        in_specs=[hbm, hbm, hbm, vmem, vmem, pl.BlockSpec(memory_space=pltpu.SMEM), vmem],
        out_specs=vmem,
        scratch_shapes=scratch,
        compiler_params=pltpu.CompilerParams(
            collective_id=0, has_side_effects=True, vmem_limit_bytes=56 * 2**20
        ),
        name="solve",
    )(
        diagonal_tiles,
        coupling_tiles,
        jacobi_inverse,
        column_part.T,
        column_tile.T,
        neighbours,
        right_side,
    )
    out = jax.ShapeDtypeStruct(right_side.shape, F32)
    return pl.pallas_call(
        split, out_shape=(out, out), in_specs=[vmem], out_specs=(vmem, vmem), name="split"
    )(both)


def solution(mesh):
    in_specs = (
        P(("groups", "rows", "sub"), None, None),
        P(("groups", "rows", "sub"), "cols", None, None),
        P(("groups", "rows", "sub"), "cols"),
        P(("groups", "rows", "sub"), "cols"),
        P("groups", None),
        P(("groups", "rows", "sub"), None),
        P(("groups", "rows", "sub"), None, None),
    )
    out_specs = (P(("groups", "rows", "sub"), None), P(("groups", "rows", "sub"), None))
    return jax.shard_map(
        on_device, mesh=mesh, in_specs=in_specs, out_specs=out_specs, check_vma=False
    )
```

```python
import functools

import jax
import jax.numpy as jnp
from jax import lax
from jax.experimental import pallas as pl
from jax.experimental.pallas import tpu as pltpu
from jax.sharding import PartitionSpec as P

MESH = pl.DeviceIdType.MESH
REACH = 2
APPLIES = 4
SUBLANES = 8
F32 = jnp.float32


def offsets_of(count):
    wanted = {d % count for d in range(-REACH, REACH + 1)} | {count // 2}
    return sorted(wanted)


def kernel(
    sizes,
    diag_hbm,
    coup_hbm,
    jac_hbm,
    part_ref,
    tile_ref,
    near_ref,
    right_ref,
    out_ref,
    diag,
    coup,
    jac,
    one_hot,
    prod,
    dprod,
    vec,
    landed,
    recv,
    dots,
    dots_recv,
    load_sem,
    send_sem,
    recv_sem,
    dots_send_sem,
    dots_recv_sem,
):
    n_rows, n_cols, n_sub = sizes
    offsets = offsets_of(n_rows)
    slots = len(offsets)
    rows_dev, slot_count, width, _ = coup.shape
    half_rows = slots * rows_dev
    chunk = rows_dev * SUBLANES
    row = lax.axis_index("rows")
    col = lax.axis_index("cols")
    sub = lax.axis_index("sub")
    me = row * n_sub + sub

    loads = [
        pltpu.make_async_copy(jac_hbm, jac, load_sem.at[0]),
        pltpu.make_async_copy(diag_hbm, diag, load_sem.at[1]),
        pltpu.make_async_copy(coup_hbm, coup, load_sem.at[2]),
    ]
    for load in loads:
        load.start()

    def partner(slot):
        return lax.rem(row + offsets[slot], n_rows)

    def if_linked(slot, act):
        if offsets[slot] in (0, n_rows // 2):
            act()
        else:
            pl.when(jnp.abs(partner(slot) - row) <= REACH)(act)

    def corner(slot, step):
        return {
            "rows": partner(slot),
            "cols": lax.rem(col + step // n_sub, n_cols),
            "sub": lax.rem(sub + step % n_sub, n_sub),
        }

    barrier = pltpu.get_barrier_semaphore()

    def dot_peers():
        for step in range(1, n_rows * n_sub):
            peer = lax.rem(me + step, n_rows * n_sub)
            yield step, peer, {"rows": lax.div(peer, n_sub), "cols": col, "sub": lax.rem(peer, n_sub)}

    recv[...] = jnp.zeros_like(recv)
    for _, _, where in dot_peers():
        pl.semaphore_signal(barrier, inc=1, device_id=where, device_id_type=MESH)
    for slot in range(slots):
        for step in range(n_sub, n_cols * n_sub):

            def greet(slot=slot, step=step):
                where = corner(slot, step)
                pl.semaphore_signal(barrier, inc=1, device_id=where, device_id_type=MESH)

            if_linked(slot, greet)

    part = part_ref[...]
    tile = tile_ref[...]
    target = jnp.full(part.shape, row, jnp.int32)
    for j in range(near_ref.shape[1]):
        target = jnp.where(part == j + 1, near_ref[row, j], target)
    apart = target - row
    apart = jnp.where(apart < 0, apart + n_rows, apart)
    place = jnp.zeros(part.shape, jnp.int32)
    for slot in range(1, slots):
        place = jnp.where(apart == offsets[slot], slot, place)
    landing = place * rows_dev + tile
    for j in range(1, n_sub):
        landing = jnp.where(tile >= j * rows_dev, landing + (half_rows - rows_dev), landing)
    from_row = lax.broadcasted_iota(jnp.int32, (rows_dev, chunk), 0)
    to_lane = lax.broadcasted_iota(jnp.int32, (rows_dev, chunk), 1)
    first = from_row * SUBLANES
    spread = ((to_lane >= first) & (to_lane < first + SUBLANES)).astype(F32)
    spread_landing = jnp.dot(
        landing.astype(F32), spread, precision=lax.Precision.HIGHEST, preferred_element_type=F32
    )
    at_row = lax.broadcasted_iota(jnp.int32, (n_sub * half_rows, chunk), 0).astype(F32)
    for k in range(slot_count):
        hit = (spread_landing[k : k + 1] == at_row).astype(F32)
        one_hot[:, k * chunk : (k + 1) * chunk] = hit.astype(jnp.bfloat16)

    loads[0].wait()

    def turn(r, carry):
        jac[r] = jnp.transpose(jac[r])
        return carry

    lax.fori_loop(0, rows_dev, turn, 0, unroll=4)

    def block(e, slot, to_sub):
        at = pl.multiple_of(to_sub * half_rows + slot * rows_dev, rows_dev)
        return landed.at[e, pl.ds(at, rows_dev)]

    def owner_copy(e, slot, step):
        back = offsets.index(-offsets[slot] % n_rows)
        where = corner(slot, step)
        return pltpu.make_async_remote_copy(
            src_ref=block(e, slot, where["sub"]),
            dst_ref=recv.at[e, back, col, sub],
            send_sem=send_sem.at[e, slot, step],
            recv_sem=recv_sem.at[e, back, col, sub],
            device_id=where,
            device_id_type=MESH,
        )

    def owner_arrival(e, slot, step):
        where = corner(slot, step)
        return pltpu.make_async_remote_copy(
            src_ref=block(e, slot, where["sub"]),
            dst_ref=recv.at[e, slot, where["cols"], where["sub"]],
            send_sem=send_sem.at[e, slot, step],
            recv_sem=recv_sem.at[e, slot, where["cols"], where["sub"]],
            device_id=where,
            device_id_type=MESH,
        )

    far_first = sorted(range(slots), key=lambda s: -min(offsets[s], n_rows - offsets[s]))
    routes = [(s, c) for s in far_first for c in reversed(range(n_cols * n_sub)) if (s, c) != (0, 0)]

    def each_route(act):
        for slot, step in routes:
            if_linked(slot, functools.partial(act, slot, step))

    def dots_copy(e, step, peer, where):
        return pltpu.make_async_remote_copy(
            src_ref=dots.at[e],
            dst_ref=dots_recv.at[e, pl.ds(me, 1)],
            send_sem=dots_send_sem.at[e, step],
            recv_sem=dots_recv_sem.at[e, me],
            device_id=where,
            device_id_type=MESH,
        )

    def dots_start(e, products):
        at = lax.broadcasted_iota(jnp.int32, (1, width), 1)
        line = jnp.zeros((1, width), F32)
        for j, product in enumerate(products):
            total = jnp.sum(jnp.sum(product, axis=0, keepdims=True), axis=1, keepdims=True)
            line = jnp.where(at == j, total, line)
        dots[e] = line
        for step, peer, where in dot_peers():
            dots_copy(e, step, peer, where).start()
        dots_recv[e, pl.ds(me, 1)] = line

    def dots_finish(e, count):
        for step, peer, where in dot_peers():
            pltpu.make_async_remote_copy(
                src_ref=dots.at[e],
                dst_ref=dots_recv.at[e, pl.ds(peer, 1)],
                send_sem=dots_send_sem.at[e, step],
                recv_sem=dots_recv_sem.at[e, peer],
                device_id=where,
                device_id_type=MESH,
            ).wait_recv()
        total = jnp.sum(dots_recv[e], axis=0, keepdims=True)
        return [jnp.broadcast_to(total[:, j : j + 1], total.shape) for j in range(count)]

    def fold(product):
        return jnp.sum(product.reshape(width // SUBLANES, SUBLANES, width), axis=0)

    unroll = 8 if rows_dev % 8 == 0 else 1

    def apply(e, value):
        vec[e] = value
        if e == 0:
            loads[1].wait()
            loads[2].wait()

        def some_rows(g, carry):
            for u in range(unroll):
                r = g * unroll + u
                hat = jnp.sum(jac[r] * vec[e, pl.ds(r, 1)], axis=1, keepdims=True)
                hat = jnp.broadcast_to(hat, (width, width))
                for k in range(slot_count):
                    at = pl.multiple_of(k * chunk + r * SUBLANES, SUBLANES)
                    prod[pl.ds(at, SUBLANES)] = fold(coup[r, k] * hat)
                dprod[pl.ds(pl.multiple_of(r * SUBLANES, SUBLANES), SUBLANES)] = fold(diag[r] * hat)
            return carry

        lax.fori_loop(0, rows_dev // unroll, some_rows, 0)
        rest = prod[...]
        out = None
        for _ in range(3):
            piece = rest.astype(jnp.bfloat16)
            rest = rest - piece.astype(F32)
            term = jnp.dot(one_hot[...], piece, preferred_element_type=F32)
            out = term if out is None else out + term
        landed[e] = out
        if e == 0:
            greetings = n_rows * n_sub - 1
            for slot in range(slots):
                linked = 1
                if offsets[slot] not in (0, n_rows // 2):
                    linked = (jnp.abs(partner(slot) - row) <= REACH).astype(jnp.int32)
                greetings = greetings + (n_cols - 1) * n_sub * linked
            pl.semaphore_wait(barrier, greetings)
        each_route(lambda slot, step: owner_copy(e, slot, step).start())
        recv[e, 0, col, sub] = landed[e, pl.ds(pl.multiple_of(sub * half_rows, rows_dev), rows_dev)]
        own = jnp.sum(dprod[...].reshape(rows_dev, SUBLANES, width), axis=1)
        each_route(lambda slot, step: owner_arrival(e, slot, step).wait_recv())
        for slot in range(slots):
            for c in range(n_cols):
                for s in range(n_sub):
                    own = own + recv[e, slot, c, s]
        return own

    shadow = right_ref[...]
    image = apply(0, shadow)
    dots_start(0, [shadow * shadow, shadow * image])
    second = apply(1, image)
    rho, shadow_image = dots_finish(0, 2)
    alpha = rho / shadow_image
    half = shadow - alpha * image
    twice = image - alpha * second
    dots_start(1, [twice * half, twice * twice, shadow * half, shadow * twice])
    third = apply(2, twice)
    cross, square, shadow_half, shadow_twice = dots_finish(1, 4)
    omega = cross / square
    rho_next = shadow_half - omega * shadow_twice
    beta = rho_next / rho * (alpha / omega)
    residual = half - omega * twice
    search = residual + beta * (shadow - omega * image)
    residual_image = twice - omega * third
    image = residual_image + beta * (image - omega * second)
    dots_start(2, [shadow * image])
    fourth = apply(3, image)
    alpha_next = rho_next / dots_finish(2, 1)[0]
    half_next = residual - alpha_next * image
    twice = residual_image - alpha_next * fourth
    dots_start(3, [twice * half_next, twice * twice])

    vec[0] = alpha * shadow + omega * half + alpha_next * search
    vec[1] = half_next
    at_lane = lax.broadcasted_iota(jnp.int32, (width, width), 1)

    def hats(r, carry):
        for j in range(2):
            hat = jnp.sum(jac[r] * vec[j, pl.ds(r, 1)], axis=1, keepdims=True)
            carry = jnp.where(at_lane == j * rows_dev + r, hat, carry)
        return carry

    hat = lax.fori_loop(0, rows_dev, hats, jnp.zeros((width, width), F32), unroll=4)
    hat = jnp.transpose(hat)
    cross, square = dots_finish(3, 2)
    omega = cross / square
    out_ref[:rows_dev] = hat[:rows_dev] + omega * hat[rows_dev : 2 * rows_dev]
    out_ref[rows_dev:] = half_next - omega * twice

    for e in range(APPLIES):
        each_route(lambda slot, step: owner_copy(e, slot, step).wait_send())
        for step, peer, where in dot_peers():
            dots_copy(e, step, peer, where).wait_send()


def split(both_ref, sol_ref, res_ref):
    rows_dev = sol_ref.shape[0]
    sol_ref[...] = both_ref[:rows_dev]
    res_ref[...] = both_ref[rows_dev:]


def on_device(
    diagonal_tiles, coupling_tiles, column_part, column_tile, neighbours, right_side, jacobi_inverse
):
    n_rows, n_cols, n_sub = (lax.axis_size(a) for a in ("rows", "cols", "sub"))
    slots = len(offsets_of(n_rows))
    rows_dev, slot_count, width, _ = coupling_tiles.shape
    half_rows = slots * rows_dev
    chunk = rows_dev * SUBLANES
    peers = n_rows * n_sub
    hbm = pl.BlockSpec(memory_space=pl.ANY)
    vmem = pl.BlockSpec(memory_space=pltpu.VMEM)
    dma = pltpu.SemaphoreType.DMA
    scratch = [
        pltpu.VMEM(diagonal_tiles.shape, F32),
        pltpu.VMEM(coupling_tiles.shape, F32),
        pltpu.VMEM(jacobi_inverse.shape, F32),
        pltpu.VMEM((n_sub * half_rows, slot_count * chunk), jnp.bfloat16),
        pltpu.VMEM((slot_count * chunk, width), F32),
        pltpu.VMEM((chunk, width), F32),
        pltpu.VMEM((APPLIES, rows_dev, width), F32),
        pltpu.VMEM((APPLIES, n_sub * half_rows, width), F32),
        pltpu.VMEM((APPLIES, slots, n_cols, n_sub, rows_dev, width), F32),
        pltpu.VMEM((APPLIES, 1, width), F32),
        pltpu.VMEM((APPLIES, peers, width), F32),
        dma((3,)),
        dma((APPLIES, slots, n_cols * n_sub)),
        dma((APPLIES, slots, n_cols, n_sub)),
        dma((APPLIES, peers)),
        dma((APPLIES, peers)),
    ]
    both = pl.pallas_call(
        functools.partial(kernel, (n_rows, n_cols, n_sub)),
        out_shape=jax.ShapeDtypeStruct((2 * rows_dev, width), F32),
        in_specs=[hbm, hbm, hbm, vmem, vmem, pl.BlockSpec(memory_space=pltpu.SMEM), vmem],
        out_specs=vmem,
        scratch_shapes=scratch,
        compiler_params=pltpu.CompilerParams(
            collective_id=0, has_side_effects=True, vmem_limit_bytes=56 * 2**20
        ),
        name="solve",
    )(
        diagonal_tiles,
        coupling_tiles,
        jacobi_inverse,
        column_part.T,
        column_tile.T,
        neighbours,
        right_side,
    )
    out = jax.ShapeDtypeStruct(right_side.shape, F32)
    return pl.pallas_call(
        split, out_shape=(out, out), in_specs=[vmem], out_specs=(vmem, vmem), name="split"
    )(both)


def solution(mesh):
    in_specs = (
        P(("groups", "rows", "sub"), None, None),
        P(("groups", "rows", "sub"), "cols", None, None),
        P(("groups", "rows", "sub"), "cols"),
        P(("groups", "rows", "sub"), "cols"),
        P("groups", None),
        P(("groups", "rows", "sub"), None),
        P(("groups", "rows", "sub"), None, None),
    )
    out_specs = (P(("groups", "rows", "sub"), None), P(("groups", "rows", "sub"), None))
    return jax.shard_map(
        on_device, mesh=mesh, in_specs=in_specs, out_specs=out_specs, check_vma=False
    )
```
